256 devices in a mesh: dp: 32 (over x, z), expert: 8 (over y, core).
Axes of the slice: x: 4, y: 4, z: 8, core: 2. Of those that a mesh axis runs over, the one named last changes fastest.
Arguments:
- tokens: bfloat16 [1024, 2048], P('expert'), may hold values from -6 to 6
- cotangent: bfloat16 [1024, 2048], P('expert'), may hold values from -0.75 to 0.75
- router_logits: float32 [1024, 2], P('expert'), may hold values from -6 to 6
- routes: int32 [1024, 2], P('expert'), may hold values from 0 to 7, all different within a row; in each aligned block of 128 rows (0 to 127, 128 to 255, ...) at most 48 rows name the same one
- gate_weight: bfloat16 [8, 7168, 2048], P('expert', 'dp'), may hold values from -0.125 to 0.125
- up_weight: bfloat16 [8, 7168, 2048], P('expert', 'dp'), may hold values from -0.125 to 0.125
- down_weight: bfloat16 [8, 7168, 2048], P('expert', 'dp'), may hold values from -0.0625 to 0.0625
- dir_gate: bfloat16 [8, 7168, 2048], P('expert', 'dp'), may hold values from -0.125 to 0.125
- dir_up: bfloat16 [8, 7168, 2048], P('expert', 'dp'), may hold values from -0.125 to 0.125
- dir_down: bfloat16 [8, 7168, 2048], P('expert', 'dp'), may hold values from -0.0625 to 0.0625
Outputs:
- mixed: bfloat16 [1024, 2048], P('expert')
- hvp_gate: float32 [8, 7168, 2048], P('expert', 'dp')
- hvp_up: float32 [8, 7168, 2048], P('expert', 'dp')
- hvp_down: float32 [8, 7168, 2048], P('expert', 'dp')
The draws below stay inside these ranges and needn't reach their ends.
Inputs may be any that keep to these rules, and one draw needn't show every extreme that they name: `routes`: each row names 2 different experts; among the 128 rows of one index of the expert axis no expert is named more than 48 times, and in every draw some block names some expert exactly 48 times.
All inputs are finite; a program needn't handle non-finite values.
Results may differ from the reference program's by a relative error of at most 0.0074.
Values may be sent and summed in bfloat16 or wider, within the bound.
A program may use at most 64 MiB of HBM per device.

```python
import math
import jax
import jax.numpy as jnp
import numpy as np
from jax import lax

D = 2048
FF = 7168
TOP = 2
TOK_DEV = 128
EXPERTS = 8
CAP = 48
TOKENS = 1024


def levels(own_key, extent, shards, least, largest):
    loudness, own = 1.0, jax.random.fold_in(own_key, 6)
    for position, blocks in shards:
        heights = jnp.exp(jax.random.uniform(jax.random.fold_in(own, position), (blocks,), jnp.float32, least / len(shards), largest / len(shards)))
        loudness = loudness * jnp.repeat(heights, extent[position] // blocks).reshape([-1 if axis == position else 1 for axis in range(len(extent))])
    return loudness


def assign_block(key, own, number, rows, amount, top, most, lean):
    order = jax.random.permutation(key, amount)
    crowded, usual = shares(amount, rows * top, most, lean, True), shares(amount, rows * top, most, lean, False)
    places = jnp.arange(amount)

    def named(lengths, rotation):
        used = int((lengths > 0).sum())
        fixed = max(1, used // 4)
        moved = fixed + (places - fixed + rotation * (used - fixed)) % max(1, amount - fixed)
        return jnp.zeros((amount,), jnp.int32).at[order[jnp.where(places < fixed, places, moved)]].set(jnp.asarray(lengths, jnp.int32))

    lengths = jnp.where(number % 4 == 0, named(crowded, number // 4), named(usual, number - number // 4 - 1))
    mixed = jax.random.permutation(jax.random.fold_in(own, 3), amount)
    source_of, sink = mixed[0:amount // 2 * 2:2], mixed[1:amount // 2 * 2:2]
    room = jnp.minimum(lengths[source_of] - 1, most - lengths[sink]) // 2
    room = jnp.where((source_of == order[0]) | (sink == order[0]) | (lengths[sink] == 0), 0, jnp.maximum(room, 0))
    moved = jax.random.randint(jax.random.fold_in(own, 4), (amount // 2,), 0, 1 << 20) % (room + 1)
    lengths = lengths.at[source_of].add(-moved).at[sink].add(moved)
    labels = jnp.searchsorted(jnp.cumsum(lengths), jnp.arange(rows * top), side="right").astype(jnp.int32)
    grid = labels.reshape(top, rows).T
    grid = grid[jax.random.permutation(jax.random.fold_in(own, 1), rows)]
    rotation = jax.random.randint(jax.random.fold_in(own, 2), (rows, 1), 0, top)
    return jnp.take_along_axis(grid, (jnp.arange(top)[None, :] + rotation) % top, axis=1)


def shares(count, total, reach, skew, full):
    portions = [(1 << 20) // math.isqrt(grade ** skew) + 1 for grade in range(1, count + 1)]
    largest = reach if full else min(reach, max(-(-total // count), total * portions[0] // sum(portions)))
    least = 1 if total - largest >= count - 1 else 0
    holding, spare = [largest] + [least] * (count - 1), total - largest - least * (count - 1)
    while spare > 0:
        candidates = [i for i in range(1, count) if holding[i] < largest] or [i for i in range(1, count) if holding[i] < reach]
        whole, left = sum([portions[i] for i in candidates]), spare
        for i in candidates:
            extra = min(reach - holding[i], max(1, left * portions[i] // whole), spare)
            holding[i] = holding[i] + extra
            spare = spare - extra
    return np.array(holding)


def gaussian(key, shape, width, most, shards=(), kind=jnp.bfloat16):
    array = width * jax.random.normal(key, shape, jnp.float32)
    if shards:
        array = array * levels(key, shape, shards, -0.22, 0.18)
    return jnp.clip(array, -most, most).astype(kind)


def setup_inputs(seed: int = 0) -> dict:
    seeds = jax.random.split(jax.random.key(seed), 11)
    tokens = gaussian(seeds[0], (TOKENS, D), 1.0, 6.0, ((0, 8),))
    cotangent = gaussian(seeds[1], (TOKENS, D), 0.125, 0.75, ((0, 8),))
    router_logits = gaussian(seeds[2], (TOKENS, TOP), 1.0, 6.0, ((0, 8),), jnp.float32)
    routes_keys = jax.random.split(jax.random.fold_in(seeds[3], 1), TOKENS // TOK_DEV)
    routes_turns = jax.random.permutation(jax.random.fold_in(seeds[3], 3), TOKENS // TOK_DEV)
    routes = jax.vmap(lambda own, number: assign_block(jax.random.fold_in(seeds[3], 2), own, number, TOK_DEV, EXPERTS, TOP, CAP, 2))(routes_keys, routes_turns).reshape((TOKENS, TOP))
    gate_weight = gaussian(seeds[4], (EXPERTS, FF, D), D ** -0.5, 0.125, ((0, 8), (1, 32)))
    up_weight = gaussian(seeds[5], (EXPERTS, FF, D), D ** -0.5, 0.125, ((0, 8), (1, 32)))
    down_weight = gaussian(seeds[6], (EXPERTS, FF, D), FF ** -0.5, 0.0625, ((0, 8), (1, 32)))
    dir_gate = gaussian(seeds[7], (EXPERTS, FF, D), D ** -0.5, 0.125, ((0, 8), (1, 32)))
    dir_up = gaussian(seeds[8], (EXPERTS, FF, D), D ** -0.5, 0.125, ((0, 8), (1, 32)))
    dir_down = gaussian(seeds[9], (EXPERTS, FF, D), FF ** -0.5, 0.0625, ((0, 8), (1, 32)))
    return dict(tokens=tokens, cotangent=cotangent, router_logits=router_logits, routes=routes, gate_weight=gate_weight, up_weight=up_weight, down_weight=down_weight, dir_gate=dir_gate, dir_up=dir_up, dir_down=dir_down)


def derivatives(preact):
    sigmoid_value = jax.nn.sigmoid(preact)
    slope_one = sigmoid_value * (1.0 + preact * (1.0 - sigmoid_value))
    slope_two = sigmoid_value * (1.0 - sigmoid_value) * (2.0 + preact * (1.0 - 2.0 * sigmoid_value))
    return preact * sigmoid_value, slope_one, slope_two


def project(left_rows, matrix):
    return jnp.einsum("rd,hd->rh", left_rows, matrix, preferred_element_type=jnp.float32)


def outer_sum(left_rows, right_rows):
    return jnp.einsum("rh,rd->hd", left_rows, right_rows, preferred_element_type=jnp.float32)


def block_terms(weights, token_rows, cot_rows):
    gate_mat, up_mat, down_mat, gate_dir, up_dir, down_dir = weights
    preact = project(token_rows, gate_mat)
    up_value = project(token_rows, up_mat)
    back_grad = project(cot_rows, down_mat)
    tang_gate = project(token_rows, gate_dir)
    tang_up = project(token_rows, up_dir)
    back_tang = project(cot_rows, down_dir)
    silu_value, slope_one, slope_two = derivatives(preact)
    hidden = (silu_value * up_value).astype(jnp.bfloat16)
    silu_tang = slope_one * tang_gate
    hidden_tang = (silu_tang * up_value + silu_value * tang_up).astype(jnp.bfloat16)
    resid_gate = ((back_tang * up_value + back_grad * tang_up) * slope_one + back_grad * up_value * slope_two * tang_gate).astype(jnp.bfloat16)
    resid_up = (back_tang * silu_value + back_grad * silu_tang).astype(jnp.bfloat16)
    return hidden, outer_sum(resid_gate, token_rows), outer_sum(resid_up, token_rows), outer_sum(hidden_tang, cot_rows)


def reference(tokens, cotangent, router_logits, routes, gate_weight, up_weight, down_weight, dir_gate, dir_up, dir_down):
    sources = TOKENS // TOK_DEV
    gate_first = jax.nn.sigmoid(router_logits[:, 0] - router_logits[:, 1])
    gate_prob = jnp.stack([gate_first, 1.0 - gate_first], axis=1)
    onehot = (routes.reshape(sources, TOK_DEV * TOP)[:, :, None] == jnp.arange(EXPERTS, dtype=jnp.int32)[None, None, :]).astype(jnp.int32)
    earlier = jnp.cumsum(onehot, axis=1) - onehot
    slot_pos = jnp.sum(earlier * onehot, axis=2).reshape(TOKENS, TOP)
    source = (jnp.arange(TOKENS, dtype=jnp.int32) // TOK_DEV)[:, None]
    slot_index = ((routes * sources + source) * CAP + slot_pos).reshape(-1).astype(jnp.int32)
    scaled = (gate_prob[:, :, None] * cotangent.astype(jnp.float32)[:, None, :]).astype(jnp.bfloat16).reshape(TOKENS * TOP, D)
    repeated = jnp.repeat(tokens, TOP, axis=0)
    total_slots = EXPERTS * sources * CAP
    slot_x = jnp.zeros((total_slots, D), jnp.bfloat16).at[slot_index].set(repeated).reshape(EXPERTS, sources * CAP, D)
    slot_c = jnp.zeros((total_slots, D), jnp.bfloat16).at[slot_index].set(scaled).reshape(EXPERTS, sources * CAP, D)

    def expert_pass(operands):
        token_rows, cot_rows = operands[0], operands[1]
        weights = operands[2:]
        hidden, part_gate, part_up, part_down = block_terms(weights, token_rows, cot_rows)
        expert_out = jnp.dot(hidden, weights[2], preferred_element_type=jnp.float32).astype(jnp.bfloat16)
        return expert_out, part_gate, part_up, part_down

    expert_out, hvp_gate, hvp_up, hvp_down = lax.map(expert_pass, (slot_x, slot_c, gate_weight, up_weight, down_weight, dir_gate, dir_up, dir_down))
    picked = expert_out.reshape(total_slots, D)[slot_index].astype(jnp.float32).reshape(TOKENS, TOP, D)
    mixed = jnp.sum(gate_prob[:, :, None] * picked, axis=1).astype(jnp.bfloat16)
    return (mixed, hvp_gate, hvp_up, hvp_down)
```

```python
import functools

import jax
import jax.numpy as jnp
from jax import lax
from jax.experimental import pallas as pl
from jax.experimental.pallas import tpu as pltpu
from jax.sharding import PartitionSpec as P

MESH = pl.DeviceIdType.MESH
F32 = jnp.float32
BF16 = jnp.bfloat16
NZ = 8
NC = 2
LANES = 128


def dot_nt(left, right):
    return lax.dot_general(left, right, (((1,), (1,)), ((), ())), preferred_element_type=F32)


def dot_tn(left, right):
    return lax.dot_general(left, right, (((0,), (0,)), ((), ())), preferred_element_type=F32)


def dot_nn(left, right):
    return jnp.dot(left, right, preferred_element_type=F32)


def aligned(index, size):
    return pl.multiple_of(index * size, size)


def layer_kernel(nx, ny, cap, *refs):
    (
        tok_hbm, cot_hbm, logits_ref, routes_ref, g_hbm, u_hbm, w_hbm, vg_hbm, vu_hbm, vw_hbm,
        mixed_hbm, slotx_hbm, slotc_hbm, resid_hbm,
        tok, cot, g, u, w, vg, vu, vw,
        disp, prob_t, send_x, send_c, slot_x, slot_c,
        xsend, xrecv, xown, zsend, zrecv, ret_send, ret, mixed, resid,
        load_sem, tok_ss, tok_rs, cot_ss, cot_rs, x_ss, x_rs, z_ss, z_rs, r_ss, r_rs,
        gz_ss, gz_rs, gx_ss, gx_rs, out_sem,
    ) = refs
    tokens, width = tok.shape
    xw = width // nx
    pair = NC * cap
    rows = ny * pair

    dp = lax.axis_index("dp")
    e = lax.axis_index("expert")
    x, z = dp // NZ, dp % NZ
    y, c = e // NC, e % NC
    parity = z % NC
    away = (c + parity) % NC

    def device(dx=0, dz=0, dy=0, dc=0):
        return (((x + dx) % nx) * NZ + (z + dz) % NZ, ((y + dy) % ny) * NC + (c + dc) % NC)

    loads = []
    for number, (src, dst) in enumerate(
        [(tok_hbm, tok), (cot_hbm, cot), (g_hbm, g), (u_hbm, u), (w_hbm, w), (vg_hbm, vg), (vu_hbm, vu), (vw_hbm, vw)]
    ):
        copy = pltpu.make_async_copy(src, dst, load_sem.at[number])
        copy.start()
        loads.append(copy)

    barrier = pltpu.get_barrier_semaphore()
    peers = []
    for dx in range(1, nx):
        peers.append(dict(dx=dx))
    for dz in range(1, NZ):
        peers.append(dict(dz=dz))
    for dy in range(ny):
        for dc in range(NC):
            if dy or dc:
                peers.append(dict(dy=dy, dc=dc))
    for peer in peers:
        pl.semaphore_signal(barrier, inc=1, device_id=device(**peer), device_id_type=MESH)

    experts = ny * NC
    expert_iota = lax.broadcasted_iota(jnp.int32, (experts, tokens), 0)
    route0, route1 = routes_ref[0:1, :], routes_ref[1:2, :]
    hot0 = (expert_iota == route0).astype(F32)
    hot1 = (expert_iota == route1).astype(F32)
    before = (
        lax.broadcasted_iota(jnp.int32, (tokens, tokens), 0)
        < lax.broadcasted_iota(jnp.int32, (tokens, tokens), 1)
    ).astype(BF16)
    earlier = dot_nn((hot0 + hot1).astype(BF16), before)
    pos0 = jnp.sum(earlier * hot0, axis=0, keepdims=True).astype(jnp.int32)
    pos1 = jnp.sum(earlier * hot1, axis=0, keepdims=True).astype(jnp.int32)
    slot_iota = lax.broadcasted_iota(jnp.int32, (rows, tokens), 0)
    disp[:, :tokens] = (slot_iota == route0 * cap + pos0).astype(F32).astype(BF16)
    disp[:, tokens:] = (slot_iota == route1 * cap + pos1).astype(F32).astype(BF16)
    first = jax.nn.sigmoid(logits_ref[0:1, :] - logits_ref[1:2, :])
    prob_t[0] = jnp.transpose(jnp.broadcast_to(first, (LANES, tokens)))
    prob_t[1] = 1.0 - prob_t[0]

    pl.semaphore_wait(barrier, len(peers))

    sends = []

    def send(src, dst, ss, rs, target):
        copy = pltpu.make_async_remote_copy(
            src_ref=src, dst_ref=dst, send_sem=ss, recv_sem=rs, device_id=target, device_id_type=MESH
        )
        copy.start()
        sends.append(copy)
        return copy

    my_rows = pl.ds(aligned(e, cap), cap)
    order = [dy for dy in (1, ny - 1, 2) if dy < ny]
    order = [dy for i, dy in enumerate(order) if dy not in order[:i]] + [0]

    def dispatch(buffer, target_buffer, ss, rs, values, hot):
        copies = {}
        for dy in order:
            yy = (y + dy) % ny
            block = pl.ds(aligned(yy, pair), pair)
            buffer[block, :] = dot_nn(hot(block), values).astype(BF16)
            for dc in range(NC):
                if dy == 0 and dc == 0:
                    target_buffer[my_rows, :] = buffer[my_rows, :]
                    continue
                ee = yy * NC + (c + dc) % NC
                number = dy * NC + dc
                copies[number] = send(
                    buffer.at[pl.ds(aligned(ee, cap), cap)], target_buffer.at[my_rows],
                    ss.at[number], rs.at[number], device(dy=dy, dc=dc),
                )
        return copies

    loads[0].wait()
    tok_copies = dispatch(
        send_x, slot_x, tok_ss, tok_rs, tok[...],
        lambda block: disp[block, :tokens] + disp[block, tokens:],
    )
    loads[1].wait()
    cot_f = cot[...].astype(F32)
    scaled = jnp.concatenate(
        [(prob_t[0][:, 0:1] * cot_f).astype(BF16), (prob_t[1][:, 0:1] * cot_f).astype(BF16)], axis=0
    )
    cot_copies = dispatch(send_c, slot_c, cot_ss, cot_rs, scaled, lambda block: disp[block, :])

    for copy in loads[2:5]:
        copy.wait()

    def group_rows(dy):
        return pl.ds(aligned((y - dy) % ny, pair), pair)

    x_copies, z_copies = {}, {}

    def forward(dy):
        for dc in range(NC):
            if dy or dc:
                tok_copies[dy * NC + dc].wait_recv()
        rows_x = slot_x[group_rows(dy), :]
        pre = dot_nt(rows_x, g[...])
        up = dot_nt(rows_x, u[...])
        hidden = (pre * jax.nn.sigmoid(pre) * up).astype(BF16)
        for dx in list(range(1, nx)) + [0]:
            xx = (x + dx) % nx
            part = dot_nn(hidden, w[:, pl.ds(aligned(xx, xw), xw)])
            if dx == 0:
                xown[dy] = part
            else:
                xsend[dy, dx - 1] = part.astype(BF16)
                x_copies[dy, dx] = send(
                    xsend.at[dy, dx - 1], xrecv.at[dy, dx - 1],
                    x_ss.at[dy, dx - 1], x_rs.at[dy, dx - 1], device(dx=dx),
                )

    def reduce_x(dy):
        total = xown[dy]
        for dx in range(1, nx):
            x_copies[dy, dx].wait_recv()
            total = total + xrecv[dy, dx - 1].astype(F32)
        zsend[dy] = total.astype(BF16)
        for dz in (4, 3, 5, 2, 6, 1, 7):
            if dz >= NZ:
                continue
            zz = (z + dz) % NZ
            src = zsend.at[dy, pl.ds(aligned(zz % NC, cap), cap), pl.ds(aligned(zz // NC, LANES), LANES)]
            z_copies[dy, dz] = send(
                src, zrecv.at[dy, dz - 1], z_ss.at[dy, dz - 1], z_rs.at[dy, dz - 1], device(dz=dz)
            )

    def reduce_z(dy):
        total = zsend[dy, pl.ds(aligned(parity, cap), cap), pl.ds(aligned(z // NC, LANES), LANES)].astype(F32)
        for dz in range(1, NZ):
            z_copies[dy, dz].wait_recv()
            total = total + zrecv[dy, dz - 1].astype(F32)
        if dy == 0:
            @pl.when(away == 0)
            def _():
                ret[my_rows, :] = total.astype(BF16)

            @pl.when(away == 1)
            def _():
                ret_send[dy] = total.astype(BF16)
                ret_copy(dy).start()
        else:
            ret_send[dy] = total.astype(BF16)
            ret_copy(dy).start()

    def ret_copy(dy):
        return pltpu.make_async_remote_copy(
            src_ref=ret_send.at[dy], dst_ref=ret.at[my_rows], send_sem=r_ss.at[dy],
            recv_sem=r_rs.at[dy * NC + away],
            device_id=(dp, ((y - dy) % ny) * NC + parity), device_id_type=MESH,
        )

    groups = [0] + [dy for dy in order if dy]
    for position, dy in enumerate(groups):
        forward(dy)
        if position >= 2:
            reduce_x(groups[position - 2])
    reduce_x(groups[-2])
    for dy in groups[:-2]:
        reduce_z(dy)
    reduce_x(groups[-1])

    for copy in loads[5:8]:
        copy.wait()
    all_x = slot_x[...]
    pre = dot_nt(g[...], all_x)
    up = dot_nt(u[...], all_x)
    tang_gate = dot_nt(vg[...], all_x)
    tang_up = dot_nt(vu[...], all_x)
    copy_x = pltpu.make_async_copy(slot_x, slotx_hbm, out_sem.at[0])
    copy_x.start()

    reduce_z(groups[-2])
    reduce_z(groups[-1])

    def piece(xx, zz):
        return mixed.at[:, pl.ds(aligned(xx * (xw // LANES) + zz // NC, LANES), LANES)]

    def gather_z(dz):
        return pltpu.make_async_remote_copy(
            src_ref=piece(x, z), dst_ref=piece(x, z), send_sem=gz_ss.at[dz - 1],
            recv_sem=gz_rs.at[dz - 1], device_id=device(dz=dz), device_id_type=MESH,
        )

    @pl.when(away == 0)
    def _():
        for dy in range(ny):
            for dc in range(NC):
                if dy or dc:
                    pltpu.make_async_remote_copy(
                        src_ref=ret_send.at[dy], dst_ref=ret.at[pl.ds(aligned(((y + dy) % ny) * NC + (c + dc) % NC, cap), cap)],
                        send_sem=r_ss.at[dy], recv_sem=r_rs.at[dy * NC + dc],
                        device_id=(dp, e), device_id_type=MESH,
                    ).wait_recv()
        returned = ret[...]
        picked0 = dot_tn(disp[:, :tokens], returned)
        picked1 = dot_tn(disp[:, tokens:], returned)
        piece(x, z)[...] = (prob_t[0] * picked0 + prob_t[1] * picked1).astype(BF16)
        for dz in range(1, NZ):
            gather_z(dz).start()

    x_gathers = []
    for number in (0, 1, NZ // NC - 1, 2):
        if number >= NZ // NC or number in [n for n, _ in x_gathers]:
            continue
        back = NC * number + away
        zz = (z + NZ - back) % NZ

        def arrived(dz):
            pltpu.make_async_remote_copy(
                src_ref=piece(x, zz), dst_ref=piece(x, zz), send_sem=gz_ss.at[dz - 1],
                recv_sem=gz_rs.at[dz - 1], device_id=(dp, e), device_id_type=MESH,
            ).wait_recv()

        if number == 0:
            @pl.when(away == 1)
            def _():
                arrived(1)
        else:
            arrived(NC * number + away)
        for dx in range(1, nx):
            copy = pltpu.make_async_remote_copy(
                src_ref=piece(x, zz), dst_ref=piece(x, zz), send_sem=gx_ss.at[number, dx - 1],
                recv_sem=gx_rs.at[number, dx - 1], device_id=device(dx=dx), device_id_type=MESH,
            )
            copy.start()
            x_gathers.append((number, copy))

    for copy in cot_copies.values():
        copy.wait_recv()
    copy_c = pltpu.make_async_copy(slot_c, slotc_hbm, out_sem.at[1])
    copy_c.start()
    all_c = slot_c[...]
    back_grad = dot_nt(w[...], all_c)
    back_tang = dot_nt(vw[...], all_c)
    sig = jax.nn.sigmoid(pre)
    silu = pre * sig
    slope_one = sig * (1.0 + pre * (1.0 - sig))
    slope_two = sig * (1.0 - sig) * (2.0 + pre * (1.0 - 2.0 * sig))
    silu_tang = slope_one * tang_gate
    resid[2] = (silu_tang * up + silu * tang_up).astype(BF16)
    resid[0] = (
        (back_tang * up + back_grad * tang_up) * slope_one + back_grad * up * slope_two * tang_gate
    ).astype(BF16)
    resid[1] = (back_tang * silu + back_grad * silu_tang).astype(BF16)
    copy_r = pltpu.make_async_copy(resid, resid_hbm, out_sem.at[2])
    copy_r.start()

    for _, copy in x_gathers:
        copy.wait_recv()
    copy_m = pltpu.make_async_copy(mixed, mixed_hbm, out_sem.at[3])
    copy_m.start()

    for copy in sends:
        copy.wait_send()
    for _, copy in x_gathers:
        copy.wait_send()
    for dy in range(1, ny):
        ret_copy(dy).wait_send()

    @pl.when(away == 1)
    def _():
        ret_copy(0).wait_send()

    @pl.when(away == 0)
    def _():
        for dz in range(1, NZ):
            gather_z(dz).wait_send()

    copy_x.wait()
    copy_c.wait()
    copy_r.wait()
    copy_m.wait()


def outer_kernel(resid, slot_x, slot_c, gate, up, down):
    rows_x = slot_x[...]
    gate[...] = dot_nn(resid[0], rows_x)
    up[...] = dot_nn(resid[1], rows_x)
    down[...] = dot_nn(resid[2], slot_c[...])


def outer_sums(resid, slot_x, slot_c):
    _, hidden, rows = resid.shape
    width = slot_x.shape[1]
    step = width // 4
    out = jax.ShapeDtypeStruct((hidden, width), F32)
    column = lambda i: (0, i)
    return pl.pallas_call(
        outer_kernel,
        grid=(width // step,),
        out_shape=(out, out, out),
        in_specs=[
            pl.BlockSpec((3, hidden, rows), lambda i: (0, 0, 0)),
            pl.BlockSpec((rows, step), column),
            pl.BlockSpec((rows, step), column),
        ],
        out_specs=[pl.BlockSpec((hidden, step), column)] * 3,
    )(resid, slot_x, slot_c)


def shards(nx, ny, tokens, cotangent, router_logits, routes, *weights):
    count, width = tokens.shape
    hidden = weights[0].shape[1]
    cap = routes.shape[1] * count * 3 // (2 * ny * NC)
    pair = NC * cap
    rows = ny * pair
    xw = width // nx
    weights = [each.reshape(hidden, width) for each in weights]
    dma = pltpu.SemaphoreType.DMA
    vmem = pltpu.VMEM
    any_spec = pl.BlockSpec(memory_space=pl.ANY)
    vmem_spec = pl.BlockSpec(memory_space=pltpu.VMEM)
    sds = jax.ShapeDtypeStruct
    mixed, slot_x, slot_c, resid = pl.pallas_call(
        functools.partial(layer_kernel, nx, ny, cap),
        out_shape=(
            sds((count, width), BF16), sds((rows, width), BF16), sds((rows, width), BF16),
            sds((3, hidden, rows), BF16),
        ),
        in_specs=[any_spec, any_spec, vmem_spec, vmem_spec] + [any_spec] * 6,
        out_specs=[any_spec] * 4,
        scratch_shapes=[vmem((count, width), BF16)] * 2
        + [vmem((hidden, width), BF16)] * 6
        + [vmem((rows, 2 * count), BF16), vmem((2, count, LANES), F32)]
        + [vmem((rows, width), BF16)] * 4
        + [
            vmem((ny, nx - 1, pair, xw), BF16), vmem((ny, nx - 1, pair, xw), BF16),
            vmem((ny, pair, xw), F32), vmem((ny, pair, xw), BF16),
            vmem((ny, NZ - 1, cap, LANES), BF16), vmem((ny, cap, LANES), BF16),
            vmem((rows, LANES), BF16), vmem((count, width), BF16), vmem((3, hidden, rows), BF16),
            dma((8,)), dma((ny * NC,)), dma((ny * NC,)), dma((ny * NC,)), dma((ny * NC,)),
            dma((ny, nx - 1)), dma((ny, nx - 1)), dma((ny, NZ - 1)), dma((ny, NZ - 1)),
            dma((ny,)), dma((ny * NC,)), dma((NZ - 1,)), dma((NZ - 1,)),
            dma((NZ // NC, nx - 1)), dma((NZ // NC, nx - 1)), dma((4,)),
        ],
        compiler_params=pltpu.CompilerParams(
            collective_id=0, has_side_effects=True, vmem_limit_bytes=60 * 1024 * 1024
        ),
    )(tokens, cotangent, router_logits.T, routes.T, *weights)
    outs = outer_sums(resid, slot_x, slot_c)
    return (mixed, *(each[None] for each in outs))


def solution(mesh):
    ny = mesh.shape["expert"] // NC
    nx = mesh.shape["dp"] // NZ
    row = P("expert", None)
    mat = P("expert", "dp", None)
    return jax.shard_map(
        functools.partial(shards, nx, ny),
        mesh=mesh,
        in_specs=(row,) * 4 + (mat,) * 6,
        out_specs=(row, mat, mat, mat),
        check_vma=False,
    )
```

```python
import functools

import jax
import jax.numpy as jnp
from jax import lax
from jax.experimental import pallas as pl
from jax.experimental.pallas import tpu as pltpu
from jax.sharding import PartitionSpec as P

MESH = pl.DeviceIdType.MESH
F32 = jnp.float32
BF16 = jnp.bfloat16
NZ = 8
NC = 2
LANES = 128


def dot_nt(left, right):
    return lax.dot_general(left, right, (((1,), (1,)), ((), ())), preferred_element_type=F32)


def dot_tn(left, right):
    return lax.dot_general(left, right, (((0,), (0,)), ((), ())), preferred_element_type=F32)


def dot_nn(left, right):
    return jnp.dot(left, right, preferred_element_type=F32)


def aligned(index, size):
    return pl.multiple_of(index * size, size)


def layer_kernel(nx, ny, cap, *refs):
    (
        tok_hbm, cot_hbm, logits_hbm, routes_hbm, g_hbm, u_hbm, w_hbm, vg_hbm, vu_hbm, vw_hbm,
        mixed, hvp_gate, hvp_up, hvp_down,
        logits_ref, routes_ref, tok, cot, g, u, w, vg, vu, vw,
        disp, prob_t, send_x, send_c, slot_x, slot_c,
        xsend, xrecv, xown, zsend, zrecv, ret_send, ret,
        load_sem, tok_ss, tok_rs, cot_ss, cot_rs, x_ss, x_rs, z_ss, z_rs, r_ss, r_rs,
        gz_ss, gz_rs, gx_ss, gx_rs,
    ) = refs
    tokens, width = tok.shape
    xw = width // nx
    pair = NC * cap
    rows = ny * pair

    dp = lax.axis_index("dp")
    e = lax.axis_index("expert")
    x, z = dp // NZ, dp % NZ
    y, c = e // NC, e % NC
    parity = z % NC
    away = (c + parity) % NC

    def device(dx=0, dz=0, dy=0, dc=0):
        return (((x + dx) % nx) * NZ + (z + dz) % NZ, ((y + dy) % ny) * NC + (c + dc) % NC)

    loads = []
    for number, (src, dst) in enumerate(
        [(routes_hbm, routes_ref), (logits_hbm, logits_ref), (tok_hbm, tok), (cot_hbm, cot), (g_hbm, g), (u_hbm, u), (w_hbm, w), (vg_hbm, vg), (vu_hbm, vu), (vw_hbm, vw)]
    ):
        copy = pltpu.make_async_copy(src, dst, load_sem.at[number])
        copy.start()
        loads.append(copy)

    barrier = pltpu.get_barrier_semaphore()
    peers = []
    for dx in range(1, nx):
        peers.append(dict(dx=dx))
    for dz in range(1, NZ):
        peers.append(dict(dz=dz))
    for dy in range(ny):
        for dc in range(NC):
            if dy or dc:
                peers.append(dict(dy=dy, dc=dc))
    for peer in peers:
        pl.semaphore_signal(barrier, inc=1, device_id=device(**peer), device_id_type=MESH)

    loads[0].wait()
    loads[1].wait()
    loads = loads[2:]

    experts = ny * NC
    expert_iota = lax.broadcasted_iota(jnp.int32, (experts, tokens), 0)
    route0, route1 = routes_ref[0:1, :], routes_ref[1:2, :]
    hot0 = (expert_iota == route0).astype(F32)
    hot1 = (expert_iota == route1).astype(F32)
    before = (
        lax.broadcasted_iota(jnp.int32, (tokens, tokens), 0)
        < lax.broadcasted_iota(jnp.int32, (tokens, tokens), 1)
    ).astype(BF16)
    earlier = dot_nn((hot0 + hot1).astype(BF16), before)
    pos0 = jnp.sum(earlier * hot0, axis=0, keepdims=True).astype(jnp.int32)
    pos1 = jnp.sum(earlier * hot1, axis=0, keepdims=True).astype(jnp.int32)
    slot_iota = lax.broadcasted_iota(jnp.int32, (rows, tokens), 0)
    disp[:, :tokens] = (slot_iota == route0 * cap + pos0).astype(F32).astype(BF16)
    disp[:, tokens:] = (slot_iota == route1 * cap + pos1).astype(F32).astype(BF16)
    first = jax.nn.sigmoid(logits_ref[0:1, :] - logits_ref[1:2, :])
    prob_t[0] = jnp.transpose(jnp.broadcast_to(first, (LANES, tokens)))
    prob_t[1] = 1.0 - prob_t[0]

    sends = []

    def send(src, dst, ss, rs, target):
        copy = pltpu.make_async_remote_copy(
            src_ref=src, dst_ref=dst, send_sem=ss, recv_sem=rs, device_id=target, device_id_type=MESH
        )
        copy.start()
        sends.append(copy)
        return copy

    my_rows = pl.ds(aligned(e, cap), cap)
    order = [dy for dy in (1, ny - 1, 2) if dy < ny]
    order = [dy for i, dy in enumerate(order) if dy not in order[:i]] + [0]

    def fill(buffer, own_buffer, values, hot):
        for dy in order:
            block = pl.ds(aligned((y + dy) % ny, pair), pair)
            buffer[block, :] = dot_nn(hot(block), values).astype(BF16)
        own_buffer[my_rows, :] = buffer[my_rows, :]

    def dispatch(buffer, target_buffer, ss, rs):
        copies = {}
        for dy in order:
            for dc in range(NC):
                if dy or dc:
                    ee = (y + dy) % ny * NC + (c + dc) % NC
                    number = dy * NC + dc
                    copies[number] = send(
                        buffer.at[pl.ds(aligned(ee, cap), cap)], target_buffer.at[my_rows],
                        ss.at[number], rs.at[number], device(dy=dy, dc=dc),
                    )
        return copies

    loads[0].wait()
    fill(send_x, slot_x, tok[...], lambda block: disp[block, :tokens] + disp[block, tokens:])
    pl.semaphore_wait(barrier, len(peers))
    tok_copies = dispatch(send_x, slot_x, tok_ss, tok_rs)
    loads[1].wait()
    cot_f = cot[...].astype(F32)
    scaled = jnp.concatenate(
        [(prob_t[0][:, 0:1] * cot_f).astype(BF16), (prob_t[1][:, 0:1] * cot_f).astype(BF16)], axis=0
    )
    fill(send_c, slot_c, scaled, lambda block: disp[block, :])
    cot_copies = dispatch(send_c, slot_c, cot_ss, cot_rs)

    for copy in loads[2:5]:
        copy.wait()

    def group_rows(dy):
        return pl.ds(aligned((y - dy) % ny, pair), pair)

    x_copies, z_copies = {}, {}

    def forward(dy):
        for dc in range(NC):
            if dy or dc:
                tok_copies[dy * NC + dc].wait_recv()
        rows_x = slot_x[group_rows(dy), :]
        pre = dot_nt(rows_x, g[...])
        up = dot_nt(rows_x, u[...])
        hidden = (pre * jax.nn.sigmoid(pre) * up).astype(BF16)
        for dx in list(range(1, nx)) + [0]:
            xx = (x + dx) % nx
            part = dot_nn(hidden, w[:, pl.ds(aligned(xx, xw), xw)])
            if dx == 0:
                xown[dy] = part
            else:
                xsend[dy, dx - 1] = part.astype(BF16)
                x_copies[dy, dx] = send(
                    xsend.at[dy, dx - 1], xrecv.at[dy, dx - 1],
                    x_ss.at[dy, dx - 1], x_rs.at[dy, dx - 1], device(dx=dx),
                )

    def reduce_x(dy):
        total = xown[dy]
        for dx in range(1, nx):
            x_copies[dy, dx].wait_recv()
            total = total + xrecv[dy, dx - 1].astype(F32)
        zsend[dy] = total.astype(BF16)
        for dz in (4, 3, 5, 2, 6, 1, 7):
            if dz >= NZ:
                continue
            zz = (z + dz) % NZ
            src = zsend.at[dy, pl.ds(aligned(zz % NC, cap), cap), pl.ds(aligned(zz // NC, LANES), LANES)]
            z_copies[dy, dz] = send(
                src, zrecv.at[dy, dz - 1], z_ss.at[dy, dz - 1], z_rs.at[dy, dz - 1], device(dz=dz)
            )

    def reduce_z(dy):
        total = zsend[dy, pl.ds(aligned(parity, cap), cap), pl.ds(aligned(z // NC, LANES), LANES)].astype(F32)
        for dz in range(1, NZ):
            z_copies[dy, dz].wait_recv()
            total = total + zrecv[dy, dz - 1].astype(F32)
        if dy == 0:
            @pl.when(away == 0)
            def _():
                ret[my_rows, :] = total.astype(BF16)

            @pl.when(away == 1)
            def _():
                ret_send[dy] = total.astype(BF16)
                ret_copy(dy).start()
        else:
            ret_send[dy] = total.astype(BF16)
            ret_copy(dy).start()

    def ret_copy(dy):
        return pltpu.make_async_remote_copy(
            src_ref=ret_send.at[dy], dst_ref=ret.at[my_rows], send_sem=r_ss.at[dy],
            recv_sem=r_rs.at[dy * NC + away],
            device_id=(dp, ((y - dy) % ny) * NC + parity), device_id_type=MESH,
        )

    groups = [0] + [dy for dy in order if dy]
    for position, dy in enumerate(groups):
        forward(dy)
        if position >= 2:
            reduce_x(groups[position - 2])
    reduce_x(groups[-2])
    for dy in groups[:-2]:
        reduce_z(dy)
    reduce_x(groups[-1])

    for copy in loads[5:8]:
        copy.wait()
    all_x = slot_x[...]
    pre = dot_nt(g[...], all_x)
    up = dot_nt(u[...], all_x)
    tang_gate = dot_nt(vg[...], all_x)
    tang_up = dot_nt(vu[...], all_x)

    reduce_z(groups[-2])
    reduce_z(groups[-1])

    def piece(xx, zz):
        return mixed.at[:, pl.ds(aligned(xx * (xw // LANES) + zz // NC, LANES), LANES)]

    def gather_z(dz):
        return pltpu.make_async_remote_copy(
            src_ref=piece(x, z), dst_ref=piece(x, z), send_sem=gz_ss.at[dz - 1],
            recv_sem=gz_rs.at[dz - 1], device_id=device(dz=dz), device_id_type=MESH,
        )

    @pl.when(away == 0)
    def _():
        for dy in range(ny):
            for dc in range(NC):
                if dy or dc:
                    pltpu.make_async_remote_copy(
                        src_ref=ret_send.at[dy], dst_ref=ret.at[pl.ds(aligned(((y + dy) % ny) * NC + (c + dc) % NC, cap), cap)],
                        send_sem=r_ss.at[dy], recv_sem=r_rs.at[dy * NC + dc],
                        device_id=(dp, e), device_id_type=MESH,
                    ).wait_recv()
        returned = ret[...]
        picked0 = dot_tn(disp[:, :tokens], returned)
        picked1 = dot_tn(disp[:, tokens:], returned)
        piece(x, z)[...] = (prob_t[0] * picked0 + prob_t[1] * picked1).astype(BF16)
        for dz in range(1, NZ):
            gather_z(dz).start()

    x_gathers = []
    for number in (0, 1, NZ // NC - 1, 2):
        if number >= NZ // NC or number in [n for n, _ in x_gathers]:
            continue
        back = NC * number + away
        zz = (z + NZ - back) % NZ

        def arrived(dz):
            pltpu.make_async_remote_copy(
                src_ref=piece(x, zz), dst_ref=piece(x, zz), send_sem=gz_ss.at[dz - 1],
                recv_sem=gz_rs.at[dz - 1], device_id=(dp, e), device_id_type=MESH,
            ).wait_recv()

        if number == 0:
            @pl.when(away == 1)
            def _():
                arrived(1)
        else:
            arrived(NC * number + away)
        for dx in range(1, nx):
            copy = pltpu.make_async_remote_copy(
                src_ref=piece(x, zz), dst_ref=piece(x, zz), send_sem=gx_ss.at[number, dx - 1],
                recv_sem=gx_rs.at[number, dx - 1], device_id=device(dx=dx), device_id_type=MESH,
            )
            copy.start()
            x_gathers.append((number, copy))

    for copy in cot_copies.values():
        copy.wait_recv()
    all_c = slot_c[...]
    back_grad = dot_nt(w[...], all_c)
    back_tang = dot_nt(vw[...], all_c)
    sig = jax.nn.sigmoid(pre)
    silu = pre * sig
    slope_one = sig * (1.0 + pre * (1.0 - sig))
    slope_two = sig * (1.0 - sig) * (2.0 + pre * (1.0 - 2.0 * sig))
    silu_tang = slope_one * tang_gate
    def outer(left, right, target):
        left = left.astype(BF16)
        half = width // 2
        for part in range(2):
            columns = pl.ds(part * half, half)
            target[:, columns] = dot_nn(left, right[:, columns])

    outer(silu_tang * up + silu * tang_up, slot_c, hvp_down)
    outer(back_tang * silu + back_grad * silu_tang, slot_x, hvp_up)
    outer(
        (back_tang * up + back_grad * tang_up) * slope_one + back_grad * up * slope_two * tang_gate,
        slot_x, hvp_gate,
    )

    for _, copy in x_gathers:
        copy.wait_recv()

    for copy in sends:
        copy.wait_send()
    for _, copy in x_gathers:
        copy.wait_send()
    for dy in range(1, ny):
        ret_copy(dy).wait_send()

    @pl.when(away == 1)
    def _():
        ret_copy(0).wait_send()

    @pl.when(away == 0)
    def _():
        for dz in range(1, NZ):
            gather_z(dz).wait_send()


def store_kernel(*refs):
    *arrays, sems = refs
    half = len(arrays) // 2
    copies = [
        pltpu.make_async_copy(arrays[i], arrays[half + i], sems.at[i]) for i in range(half)
    ]
    for copy in copies:
        copy.start()
    for copy in copies:
        copy.wait()


def shards(nx, ny, tokens, cotangent, router_logits, routes, *weights):
    count, width = tokens.shape
    hidden = weights[0].shape[1]
    cap = routes.shape[1] * count * 3 // (2 * ny * NC)
    pair = NC * cap
    rows = ny * pair
    xw = width // nx
    weights = [each.reshape(hidden, width) for each in weights]
    dma = pltpu.SemaphoreType.DMA
    vmem = pltpu.VMEM
    any_spec = pl.BlockSpec(memory_space=pl.ANY)
    hbm_spec = pl.BlockSpec(memory_space=pltpu.HBM)
    vmem_spec = pl.BlockSpec(memory_space=pltpu.VMEM)
    sds = jax.ShapeDtypeStruct
    hvp = sds((hidden, width), F32)
    shapes = (sds((count, width), BF16), hvp, hvp, hvp)
    args = (tokens, cotangent, router_logits.T, routes.T, *weights)
    args = [pltpu.with_memory_space_constraint(each, pltpu.HBM) for each in args]
    results = pl.pallas_call(
        functools.partial(layer_kernel, nx, ny, cap),
        out_shape=tuple(pltpu.VMEM(each.shape, each.dtype) for each in shapes),
        in_specs=[hbm_spec] * 10,
        out_specs=[vmem_spec] * 4,
        scratch_shapes=[vmem(args[2].shape, F32), vmem(args[3].shape, jnp.int32)]
        + [vmem((count, width), BF16)] * 2
        + [vmem((hidden, width), BF16)] * 6
        + [vmem((rows, 2 * count), BF16), vmem((2, count, LANES), F32)]
        + [vmem((rows, width), BF16)] * 4
        + [
            vmem((ny, nx - 1, pair, xw), BF16), vmem((ny, nx - 1, pair, xw), BF16),
            vmem((ny, pair, xw), F32), vmem((ny, pair, xw), BF16),
            vmem((ny, NZ - 1, cap, LANES), BF16), vmem((ny, cap, LANES), BF16),
            vmem((rows, LANES), BF16),
            dma((10,)), dma((ny * NC,)), dma((ny * NC,)), dma((ny * NC,)), dma((ny * NC,)),
            dma((ny, nx - 1)), dma((ny, nx - 1)), dma((ny, NZ - 1)), dma((ny, NZ - 1)),
            dma((ny,)), dma((ny * NC,)), dma((NZ - 1,)), dma((NZ - 1,)),
            dma((NZ // NC, nx - 1)), dma((NZ // NC, nx - 1)),
        ],
        compiler_params=pltpu.CompilerParams(
            collective_id=0, has_side_effects=True, vmem_limit_bytes=36 * 1024 * 1024
        ),
    )(*args)
    mixed, *outs = pl.pallas_call(
        store_kernel,
        out_shape=tuple(pltpu.HBM(each.shape, each.dtype) for each in shapes),
        in_specs=[any_spec] * 4,
        out_specs=[hbm_spec] * 4,
        scratch_shapes=[dma((4,))],
        compiler_params=pltpu.CompilerParams(vmem_limit_bytes=1024 * 1024),
    )(*[pltpu.with_memory_space_constraint(each, pltpu.VMEM) for each in results])
    return (mixed, *(each[None] for each in outs))


def solution(mesh):
    ny = mesh.shape["expert"] // NC
    nx = mesh.shape["dp"] // NZ
    row = P("expert", None)
    mat = P("expert", "dp", None)
    return jax.shard_map(
        functools.partial(shards, nx, ny),
        mesh=mesh,
        in_specs=(row,) * 4 + (mat,) * 6,
        out_specs=(row, mat, mat, mat),
        check_vma=False,
    )
```

```python
import functools

import jax
import jax.numpy as jnp
from jax import lax
from jax.experimental import pallas as pl
from jax.experimental.pallas import tpu as pltpu
from jax.sharding import PartitionSpec as P

MESH = pl.DeviceIdType.MESH
F32 = jnp.float32
BF16 = jnp.bfloat16
NZ = 8
NC = 2
LANES = 128


def dot_nt(left, right):
    return lax.dot_general(left, right, (((1,), (1,)), ((), ())), preferred_element_type=F32)


def dot_tn(left, right):
    return lax.dot_general(left, right, (((0,), (0,)), ((), ())), preferred_element_type=F32)


def dot_nn(left, right):
    return jnp.dot(left, right, preferred_element_type=F32)


def aligned(index, size):
    return pl.multiple_of(index * size, size)


def layer_kernel(nx, ny, cap, *refs):
    (
        tok_hbm, cot_hbm, logits_hbm, routes_hbm, g_hbm, u_hbm, w_hbm, vg_hbm, vu_hbm, vw_hbm,
        mixed, hvp_gate, hvp_up, hvp_down,
        logits_ref, routes_ref, tok, cot, g, u, w, vg, vu, vw,
        disp, prob_t, send_x, send_c, slot_x, slot_c,
        xsend, xrecv, xown, zsend, final,
        load_sem, send_sem, tok_rs, x_rs, one_rs, gz_rs,
    ) = refs
    tokens, width = tok.shape
    xw = width // nx
    pair = NC * cap
    rows = ny * pair

    dp = lax.axis_index("dp")
    e = lax.axis_index("expert")
    x, z = dp // NZ, dp % NZ
    y, c = e // NC, e % NC
    parity = z % NC
    away = (c + parity) % NC

    def device(dx=0, dz=0, dy=0, dc=0):
        return (((x + dx) % nx) * NZ + (z + dz) % NZ, ((y + dy) % ny) * NC + (c + dc) % NC)

    loads = []
    for number, (src, dst) in enumerate(
        [(routes_hbm, routes_ref), (logits_hbm, logits_ref), (tok_hbm, tok), (cot_hbm, cot), (g_hbm, g), (u_hbm, u), (w_hbm, w), (vg_hbm, vg), (vu_hbm, vu), (vw_hbm, vw)]
    ):
        copy = pltpu.make_async_copy(src, dst, load_sem.at[number])
        copy.start()
        loads.append(copy)

    barrier = pltpu.get_barrier_semaphore()
    peers = []
    for dx in range(1, nx):
        peers.append(dict(dx=dx))
    for dz in range(1, NZ):
        peers.append(dict(dz=dz))
    for dy in range(ny):
        for dc in range(NC):
            if dy or dc:
                peers.append(dict(dy=dy, dc=dc))
    for peer in peers:
        pl.semaphore_signal(barrier, inc=1, device_id=device(**peer), device_id_type=MESH)

    loads[0].wait()
    loads[1].wait()
    loads = loads[2:]

    experts = ny * NC
    expert_iota = lax.broadcasted_iota(jnp.int32, (experts, tokens), 0)
    route0, route1 = routes_ref[0:1, :], routes_ref[1:2, :]
    hot0 = (expert_iota == route0).astype(F32)
    hot1 = (expert_iota == route1).astype(F32)
    before = (
        lax.broadcasted_iota(jnp.int32, (tokens, tokens), 0)
        < lax.broadcasted_iota(jnp.int32, (tokens, tokens), 1)
    ).astype(BF16)
    earlier = dot_nn((hot0 + hot1).astype(BF16), before)
    pos0 = jnp.sum(earlier * hot0, axis=0, keepdims=True).astype(jnp.int32)
    pos1 = jnp.sum(earlier * hot1, axis=0, keepdims=True).astype(jnp.int32)
    slot_iota = lax.broadcasted_iota(jnp.int32, (rows, tokens), 0)
    disp[:, :tokens] = (slot_iota == route0 * cap + pos0).astype(F32).astype(BF16)
    disp[:, tokens:] = (slot_iota == route1 * cap + pos1).astype(F32).astype(BF16)
    first = jax.nn.sigmoid(logits_ref[0:1, :] - logits_ref[1:2, :])
    prob_t[0] = jnp.transpose(jnp.broadcast_to(first, (LANES, tokens)))
    prob_t[1] = 1.0 - prob_t[0]

    cot_rs, far_rs, fin_rs, gx_rs = (one_rs.at[number] for number in range(4))
    tok_ss, cot_ss, x_ss, fin_ss, far_ss, own_ss, gz_ss, gx_ss, tokf_ss = (
        send_sem.at[number] for number in range(9)
    )

    def remote(src, dst, ss, rs, target):
        return pltpu.make_async_remote_copy(
            src_ref=src, dst_ref=dst, send_sem=ss, recv_sem=rs, device_id=target, device_id_type=MESH
        )

    def send(*args):
        remote(*args).start()

    def sent(ref, ss):
        remote(ref, ref, ss, gx_rs, (dp, e)).wait_send()

    def received(ref, rs):
        remote(ref, ref, gx_ss, rs, (dp, e)).wait_recv()

    my_rows = pl.ds(aligned(e, cap), cap)
    order = [dy for dy in (1, ny - 1, 2) if dy < ny]
    order = [dy for i, dy in enumerate(order) if dy not in order[:i]] + [0]

    def fill(buffer, own_buffer, values, hot):
        for dy in order:
            block = pl.ds(aligned((y + dy) % ny, pair), pair)
            buffer[block, :] = dot_nn(hot(block), values).astype(BF16)
        own_buffer[my_rows, :] = buffer[my_rows, :]

    far = ny // 2 if ny > 2 else 0
    share = width // NZ
    my_share = pl.ds(aligned(z, share), share)

    def arrival(dy, dc):
        return 0 if dy == far and far else 1 if dy == 0 else 2 + dc

    def dispatch(buffer, target_buffer, through_z, blocks):
        for dy, dc in blocks:
            ee = (y + dy) % ny * NC + (c + dc) % NC
            part = through_z and dy == far and far
            columns = my_share if part else pl.ds(0, width)
            send(
                buffer.at[pl.ds(aligned(ee, cap), cap), columns], target_buffer.at[my_rows, columns],
                (tokf_ss if part else tok_ss) if through_z else cot_ss,
                tok_rs.at[arrival(dy, dc)] if through_z else cot_rs, device(dy=dy, dc=dc),
            )

    near = [dy for dy in order if dy and dy != far]
    direct_order = [(0, 1)] + [(dy, dc) for dy in near + [far] if dy for dc in range(NC)]
    through_order = [(far, dc) for dc in range(NC)] if far else []
    through_order += [(0, 1)] + [(dy, dc) for dc in range(NC) for dy in near]

    loads[0].wait()
    fill(send_x, slot_x, tok[...], lambda block: disp[block, :tokens] + disp[block, tokens:])
    pl.semaphore_wait(barrier, len(peers))
    dispatch(send_x, slot_x, True, through_order)
    loads[1].wait()
    cot_f = cot[...].astype(F32)
    scaled = jnp.concatenate(
        [(prob_t[0][:, 0:1] * cot_f).astype(BF16), (prob_t[1][:, 0:1] * cot_f).astype(BF16)], axis=0
    )
    fill(send_c, slot_c, scaled, lambda block: disp[block, :])
    dispatch(send_c, slot_c, False, direct_order[:-2] if far else direct_order)

    for copy in loads[2:5]:
        copy.wait()

    z_order = [dz for dz in (4, 3, 5, 2, 6, 1, 7) if dz < NZ]

    def group_rows(dy):
        return pl.ds(aligned((y - dy) % ny, pair), pair)

    def forward(blocks):
        together = len({dy for dy, _ in blocks}) == 1
        if together:
            rows_x = slot_x[group_rows(blocks[0][0]), :]
        else:
            rows_x = jnp.concatenate(
                [slot_x[pl.ds(aligned((y - dy) % ny * NC + (c + dc) % NC, cap), cap), :] for dy, dc in blocks],
                axis=0,
            )
        pre = dot_nt(rows_x, g[...])
        up = dot_nt(rows_x, u[...])
        hidden = (pre * jax.nn.sigmoid(pre) * up).astype(BF16)
        for dx in list(range(1, nx)) + [0]:
            xx = (x + dx) % nx
            part = dot_nn(hidden, w[:, pl.ds(aligned(xx, xw), xw)])
            for number, (dy, dc) in enumerate([(blocks[0][0], 0)] if together else blocks):
                place = pl.ds(0, pair) if together else pl.ds(aligned((c + dc) % NC, cap), cap)
                value = part if together else part[number * cap : (number + 1) * cap]
                if dx == 0:
                    xown[dy, place] = value
                else:
                    xsend[dy, dx - 1, place] = value.astype(BF16)
                    send(
                        xsend.at[dy, dx - 1, place], xrecv.at[dy, dx - 1, place],
                        x_ss, x_rs.at[dy], device(dx=dx),
                    )

    def spread_far():
        received(slot_x.at[pl.ds(0, pair), pl.ds(0, share)], tok_rs.at[0])
        part = slot_x.at[group_rows(far), my_share]
        for dz in z_order:
            send(part, part, far_ss, far_rs, device(dz=dz))

    def reduce_x(dy):
        received(xrecv.at[dy], x_rs.at[dy])
        total = xown[dy]
        for dx in range(1, nx):
            total = total + xrecv[dy, dx - 1].astype(F32)
        zsend[dy] = total.astype(BF16)
        for dz in z_order:
            final_copy(dy, dz).start()
        if dy:
            final_copy(dy, 0).start()
        else:
            @pl.when(away == 1)
            def _():
                final_copy(0, 0).start()

            @pl.when(away == 0)
            def _():
                final[my_final, :] = zsend.at[final_part(0, z)][...]

    my_final = pl.ds(aligned(z * experts + e, cap), cap)

    def final_part(dy, zz):
        return (dy, pl.ds(aligned(zz % NC, cap), cap), pl.ds(aligned(zz // NC, LANES), LANES))

    def final_copy(dy, dz):
        zz = (z + dz) % NZ
        target = (x * NZ + zz, (y - dy + ny) % ny * NC + zz % NC)
        return remote(
            zsend.at[final_part(dy, zz)], final.at[my_final], fin_ss if dy or dz else own_ss, fin_rs, target
        )

    received(slot_x.at[pl.ds(0, cap)], tok_rs.at[1])
    forward([(0, 0), (0, 1)])
    if far:
        spread_far()
    for dc in range(NC):
        received(slot_x.at[pl.ds(0, cap * len(near))], tok_rs.at[2 + dc])
        forward([(dy, dc) for dy in near])
        if dc == 0:
            reduce_x(0)
        elif far:
            dispatch(send_c, slot_c, False, direct_order[-2:-1])
    if far:
        received(slot_x.at[pl.ds(0, pair), pl.ds(0, width - share)], far_rs)
        forward([(far, 0), (far, 1)])
    for dy in near:
        reduce_x(dy)

    for copy in loads[5:8]:
        copy.wait()
    all_x = slot_x[...]
    pre = dot_nt(g[...], all_x)
    up = dot_nt(u[...], all_x)
    tang_gate = dot_nt(vg[...], all_x)
    tang_up = dot_nt(vu[...], all_x)

    if far:
        reduce_x(far)
        dispatch(send_c, slot_c, False, direct_order[-1:])

    def piece(xx, zz):
        return mixed.at[:, pl.ds(aligned(xx * (xw // LANES) + zz // NC, LANES), LANES)]

    def gather_z(dz):
        return pltpu.make_async_remote_copy(
            src_ref=piece(x, z), dst_ref=piece(x, z), send_sem=gz_ss,
            recv_sem=gz_rs.at[dz - 1], device_id=device(dz=dz), device_id_type=MESH,
        )

    @pl.when(away == 0)
    def _():
        received(final.at[pl.ds(0, NZ * rows - cap)], fin_rs)
        total = final[pl.ds(0, rows), :].astype(F32)
        for zz in range(1, NZ):
            total = total + final[pl.ds(zz * rows, rows), :].astype(F32)
        returned = total.astype(BF16)
        picked0 = dot_tn(disp[:, :tokens], returned)
        picked1 = dot_tn(disp[:, tokens:], returned)
        piece(x, z)[...] = (prob_t[0] * picked0 + prob_t[1] * picked1).astype(BF16)
        for dz in range(1, NZ):
            gather_z(dz).start()

    def pass_on(number, source=None):
        back = NC * number + (away if source is None else 1 - source)
        zz = (z + NZ - back) % NZ
        part = piece(x, zz)
        if number or not source:
            received(part, gz_rs.at[back - 1])
        for dx in range(1, nx):
            send(part, part, gx_ss, gx_rs, device(dx=dx))

    @pl.when(away == 0)
    def _():
        pass_on(0, True)

    def outer(left, right, target):
        left = left.astype(BF16)
        half = width // 2
        for part in range(2):
            columns = pl.ds(part * half, half)
            target[:, columns] = dot_nn(left, right[:, columns])

    @pl.when(away == 1)
    def _():
        pass_on(0, False)

    for number in (3, 1, 2):
        if number < NZ // NC:
            pass_on(number)

    received(slot_c.at[pl.ds(0, rows - cap)], cot_rs)
    all_c = slot_c[...]
    back_grad = dot_nt(w[...], all_c)
    back_tang = dot_nt(vw[...], all_c)
    sig = jax.nn.sigmoid(pre)
    silu = pre * sig
    slope_one = sig * (1.0 + pre * (1.0 - sig))
    slope_two = sig * (1.0 - sig) * (2.0 + pre * (1.0 - 2.0 * sig))
    silu_tang = slope_one * tang_gate
    outer(silu_tang * up + silu * tang_up, slot_c, hvp_down)
    outer(back_tang * silu + back_grad * silu_tang, slot_x, hvp_up)
    outer(
        (back_tang * up + back_grad * tang_up) * slope_one + back_grad * up * slope_two * tang_gate,
        slot_x, hvp_gate,
    )

    gathered = NZ // NC * (nx - 1) * LANES
    received(mixed.at[:, pl.ds(0, gathered)], gx_rs)

    direct = 1 + NC * len(near)
    sent(slot_x.at[pl.ds(0, direct * cap)], tok_ss)
    sent(slot_c.at[pl.ds(0, rows - cap)], cot_ss)
    if far:
        sent(slot_x.at[pl.ds(0, pair), pl.ds(0, share)], tokf_ss)
        sent(slot_x.at[pl.ds(0, pair), pl.ds(0, width - share)], far_ss)
    sent(xsend, x_ss)
    sent(final.at[pl.ds(0, (ny * NZ - 1) * cap)], fin_ss)
    sent(mixed.at[:, pl.ds(0, gathered)], gx_ss)

    @pl.when(away == 1)
    def _():
        sent(final.at[pl.ds(0, cap)], own_ss)

    @pl.when(away == 0)
    def _():
        sent(mixed.at[:, pl.ds(0, (NZ - 1) * LANES)], gz_ss)


def store_kernel(*refs):
    *arrays, sems = refs
    half = len(arrays) // 2
    copies = [
        pltpu.make_async_copy(arrays[i], arrays[half + i], sems.at[i]) for i in range(half)
    ]
    for copy in copies:
        copy.start()
    for copy in copies:
        copy.wait()


def shards(nx, ny, tokens, cotangent, router_logits, routes, *weights):
    count, width = tokens.shape
    hidden = weights[0].shape[1]
    cap = routes.shape[1] * count * 3 // (2 * ny * NC)
    pair = NC * cap
    rows = ny * pair
    xw = width // nx
    weights = [each.reshape(hidden, width) for each in weights]
    dma = pltpu.SemaphoreType.DMA
    vmem = pltpu.VMEM
    any_spec = pl.BlockSpec(memory_space=pl.ANY)
    hbm_spec = pl.BlockSpec(memory_space=pltpu.HBM)
    vmem_spec = pl.BlockSpec(memory_space=pltpu.VMEM)
    sds = jax.ShapeDtypeStruct
    hvp = sds((hidden, width), F32)
    shapes = (sds((count, width), BF16), hvp, hvp, hvp)
    args = (tokens, cotangent, router_logits.T, routes.T, *weights)
    args = [pltpu.with_memory_space_constraint(each, pltpu.HBM) for each in args]
    results = pl.pallas_call(
        functools.partial(layer_kernel, nx, ny, cap),
        out_shape=tuple(pltpu.VMEM(each.shape, each.dtype) for each in shapes),
        in_specs=[hbm_spec] * 10,
        out_specs=[vmem_spec] * 4,
        scratch_shapes=[vmem(args[2].shape, F32), vmem(args[3].shape, jnp.int32)]
        + [vmem((count, width), BF16)] * 2
        + [vmem((hidden, width), BF16)] * 6
        + [vmem((rows, 2 * count), BF16), vmem((2, count, LANES), F32)]
        + [vmem((rows, width), BF16)] * 4
        + [
            vmem((ny, nx - 1, pair, xw), BF16), vmem((ny, nx - 1, pair, xw), BF16),
            vmem((ny, pair, xw), F32), vmem((ny, pair, xw), BF16),
            vmem((NZ * rows, LANES), BF16),
            dma((10,)), dma((9,)), dma((2 + NC,)), dma((ny,)), dma((4,)), dma((NZ - 1,)),
        ],
        compiler_params=pltpu.CompilerParams(
            collective_id=0, has_side_effects=True, vmem_limit_bytes=36 * 1024 * 1024
        ),
    )(*args)
    mixed, *outs = pl.pallas_call(
        store_kernel,
        out_shape=tuple(pltpu.HBM(each.shape, each.dtype) for each in shapes),
        in_specs=[any_spec] * 4,
        out_specs=[hbm_spec] * 4,
        scratch_shapes=[dma((4,))],
        compiler_params=pltpu.CompilerParams(vmem_limit_bytes=1024 * 1024),
    )(*[pltpu.with_memory_space_constraint(each, pltpu.VMEM) for each in results])
    return (mixed, *(each[None] for each in outs))


def solution(mesh):
    ny = mesh.shape["expert"] // NC
    nx = mesh.shape["dp"] // NZ
    row = P("expert", None)
    mat = P("expert", "dp", None)
    return jax.shard_map(
        functools.partial(shards, nx, ny),
        mesh=mesh,
        in_specs=(row,) * 4 + (mat,) * 6,
        out_specs=(row, mat, mat, mat),
        check_vma=False,
    )
```

```python
import functools

import jax
import jax.numpy as jnp
from jax import lax
from jax.experimental import pallas as pl
from jax.experimental.pallas import tpu as pltpu
from jax.sharding import PartitionSpec as P

MESH = pl.DeviceIdType.MESH
F32 = jnp.float32
BF16 = jnp.bfloat16
NZ = 8
NC = 2
LANES = 128


def dot_nt(left, right):
    return lax.dot_general(left, right, (((1,), (1,)), ((), ())), preferred_element_type=F32)


def dot_tn(left, right):
    return lax.dot_general(left, right, (((0,), (0,)), ((), ())), preferred_element_type=F32)


def dot_nn(left, right):
    return jnp.dot(left, right, preferred_element_type=F32)


def aligned(index, size):
    return pl.multiple_of(index * size, size)


def layer_kernel(nx, ny, cap, *refs):
    (
        tok_hbm, cot_hbm, logits_hbm, routes_hbm, g_hbm, u_hbm, w_hbm, vg_hbm, vu_hbm, vw_hbm,
        mixed, hvp_gate, hvp_up, hvp_down,
        logits_ref, routes_ref, tok, cot, g, u, w, vg, vu, vw,
        disp, prob_t, send_x, send_c, slot_x, slot_c,
        xsend, xrecv, xown, zsend, final,
        load_sem, send_sem, tok_rs, x_rs, one_rs, gz_rs,
    ) = refs
    tokens, width = tok.shape
    xw = width // nx
    pair = NC * cap
    rows = ny * pair

    dp = lax.axis_index("dp")
    e = lax.axis_index("expert")
    x, z = dp // NZ, dp % NZ
    y, c = e // NC, e % NC
    parity = z % NC
    away = (c + parity) % NC

    def device(dx=0, dz=0, dy=0, dc=0):
        return (((x + dx) % nx) * NZ + (z + dz) % NZ, ((y + dy) % ny) * NC + (c + dc) % NC)

    loads = []
    for number, (src, dst) in enumerate(
        [(routes_hbm, routes_ref), (logits_hbm, logits_ref), (tok_hbm, tok), (cot_hbm, cot), (g_hbm, g), (u_hbm, u), (w_hbm, w), (vg_hbm, vg), (vu_hbm, vu), (vw_hbm, vw)]
    ):
        copy = pltpu.make_async_copy(src, dst, load_sem.at[number])
        copy.start()
        loads.append(copy)

    barrier = pltpu.get_barrier_semaphore()
    peers = []
    for dx in range(1, nx):
        peers.append(dict(dx=dx))
    for dz in range(1, NZ):
        peers.append(dict(dz=dz))
    for dy in range(ny):
        for dc in range(NC):
            if dy or dc:
                peers.append(dict(dy=dy, dc=dc))
    for peer in peers:
        pl.semaphore_signal(barrier, inc=1, device_id=device(**peer), device_id_type=MESH)

    loads[0].wait()
    loads[1].wait()
    loads = loads[2:]

    experts = ny * NC
    expert_iota = lax.broadcasted_iota(jnp.int32, (experts, tokens), 0)
    route0, route1 = routes_ref[0:1, :], routes_ref[1:2, :]
    hot0 = (expert_iota == route0).astype(F32)
    hot1 = (expert_iota == route1).astype(F32)
    before = (
        lax.broadcasted_iota(jnp.int32, (tokens, tokens), 0)
        < lax.broadcasted_iota(jnp.int32, (tokens, tokens), 1)
    ).astype(BF16)
    earlier = dot_nn((hot0 + hot1).astype(BF16), before)
    pos0 = jnp.sum(earlier * hot0, axis=0, keepdims=True).astype(jnp.int32)
    pos1 = jnp.sum(earlier * hot1, axis=0, keepdims=True).astype(jnp.int32)
    slot_iota = lax.broadcasted_iota(jnp.int32, (rows, tokens), 0)
    disp[:, :tokens] = (slot_iota == route0 * cap + pos0).astype(F32).astype(BF16)
    disp[:, tokens:] = (slot_iota == route1 * cap + pos1).astype(F32).astype(BF16)
    first = jax.nn.sigmoid(logits_ref[0:1, :] - logits_ref[1:2, :])
    prob_t[0] = jnp.transpose(jnp.broadcast_to(first, (LANES, tokens)))
    prob_t[1] = 1.0 - prob_t[0]

    cot_rs, far_rs, fin_rs, gx_rs = (one_rs.at[number] for number in range(4))
    tok_ss, cot_ss, x_ss, fin_ss, far_ss, own_ss, gz_ss, gx_ss, tokf_ss = (
        send_sem.at[number] for number in range(9)
    )

    def remote(src, dst, ss, rs, target):
        return pltpu.make_async_remote_copy(
            src_ref=src, dst_ref=dst, send_sem=ss, recv_sem=rs, device_id=target, device_id_type=MESH
        )

    def send(*args):
        remote(*args).start()

    def sent(ref, ss):
        remote(ref, ref, ss, gx_rs, (dp, e)).wait_send()

    def received(ref, rs):
        remote(ref, ref, gx_ss, rs, (dp, e)).wait_recv()

    my_rows = pl.ds(aligned(e, cap), cap)
    order = [dy for dy in (1, ny - 1, 2) if dy < ny]
    order = [dy for i, dy in enumerate(order) if dy not in order[:i]] + [0]

    def fill(buffer, own_buffer, values, hot):
        for dy in order:
            block = pl.ds(aligned((y + dy) % ny, pair), pair)
            buffer[block, :] = dot_nn(hot(block), values).astype(BF16)
        own_buffer[my_rows, :] = buffer[my_rows, :]

    far = ny // 2 if ny > 2 else 0
    share = width // NZ
    my_share = pl.ds(aligned(z, share), share)

    def arrival(dy, dc):
        return 0 if dy == far and far else 1 if dy == 0 else 2 + dc

    def dispatch(buffer, target_buffer, through_z, blocks):
        for dy, dc in blocks:
            ee = (y + dy) % ny * NC + (c + dc) % NC
            part = through_z and dy == far and far
            columns = my_share if part else pl.ds(0, width)
            send(
                buffer.at[pl.ds(aligned(ee, cap), cap), columns], target_buffer.at[my_rows, columns],
                (tokf_ss if part else tok_ss) if through_z else cot_ss,
                tok_rs.at[arrival(dy, dc)] if through_z else cot_rs, device(dy=dy, dc=dc),
            )

    near = [dy for dy in order if dy and dy != far]
    direct_order = [(0, 1)] + [(dy, dc) for dy in near + [far] if dy for dc in range(NC)]
    through_order = [(far, dc) for dc in range(NC)] if far else []
    through_order += [(0, 1)] + [(dy, dc) for dc in range(NC) for dy in near]

    loads[0].wait()
    fill(send_x, slot_x, tok[...], lambda block: disp[block, :tokens] + disp[block, tokens:])
    pl.semaphore_wait(barrier, len(peers))
    dispatch(send_x, slot_x, True, through_order)
    loads[1].wait()
    cot_f = cot[...].astype(F32)
    scaled = jnp.concatenate(
        [(prob_t[0][:, 0:1] * cot_f).astype(BF16), (prob_t[1][:, 0:1] * cot_f).astype(BF16)], axis=0
    )
    fill(send_c, slot_c, scaled, lambda block: disp[block, :])
    dispatch(send_c, slot_c, False, direct_order[:-2] if far else direct_order)

    for copy in loads[2:5]:
        copy.wait()

    z_order = [dz for dz in (4, 3, 5, 2, 6, 1, 7) if dz < NZ]

    def group_rows(dy):
        return pl.ds(aligned((y - dy) % ny, pair), pair)

    def forward(blocks):
        together = len({dy for dy, _ in blocks}) == 1
        if together:
            rows_x = slot_x[group_rows(blocks[0][0]), :]
        else:
            rows_x = jnp.concatenate(
                [slot_x[pl.ds(aligned((y - dy) % ny * NC + (c + dc) % NC, cap), cap), :] for dy, dc in blocks],
                axis=0,
            )
        pre = dot_nt(rows_x, g[...])
        up = dot_nt(rows_x, u[...])
        hidden = (pre * jax.nn.sigmoid(pre) * up).astype(BF16)
        for dx in list(range(1, nx)) + [0]:
            xx = (x + dx) % nx
            part = dot_nn(hidden, w[:, pl.ds(aligned(xx, xw), xw)])
            for number, (dy, dc) in enumerate([(blocks[0][0], 0)] if together else blocks):
                place = pl.ds(0, pair) if together else pl.ds(aligned((c + dc) % NC, cap), cap)
                value = part if together else part[number * cap : (number + 1) * cap]
                if dx == 0:
                    xown[dy, place] = value
                else:
                    xsend[dy, dx - 1, place] = value.astype(BF16)
                    send(
                        xsend.at[dy, dx - 1, place], xrecv.at[dy, dx - 1, place],
                        x_ss, x_rs.at[dy], device(dx=dx),
                    )

    def spread_far():
        received(slot_x.at[pl.ds(0, pair), pl.ds(0, share)], tok_rs.at[0])
        part = slot_x.at[group_rows(far), my_share]
        for dz in z_order:
            send(part, part, far_ss, far_rs, device(dz=dz))

    def reduce_x(dy):
        received(xrecv.at[dy], x_rs.at[dy])
        total = xown[dy]
        for dx in range(1, nx):
            total = total + xrecv[dy, dx - 1].astype(F32)
        zsend[dy] = total.astype(BF16)
        for dz in z_order:
            final_copy(dy, dz).start()
        if dy:
            final_copy(dy, 0).start()
        else:
            @pl.when(away == 1)
            def _():
                final_copy(0, 0).start()

            @pl.when(away == 0)
            def _():
                final[my_final, :] = zsend.at[final_part(0, z)][...]

    my_final = pl.ds(aligned(z * experts + e, cap), cap)

    def final_part(dy, zz):
        return (dy, pl.ds(aligned(zz % NC, cap), cap), pl.ds(aligned(zz // NC, LANES), LANES))

    def final_copy(dy, dz):
        zz = (z + dz) % NZ
        target = (x * NZ + zz, (y - dy + ny) % ny * NC + zz % NC)
        return remote(
            zsend.at[final_part(dy, zz)], final.at[my_final], fin_ss if dy or dz else own_ss, fin_rs, target
        )

    received(slot_x.at[pl.ds(0, cap)], tok_rs.at[1])
    forward([(0, 0), (0, 1)])
    if far:
        spread_far()
    for dc in range(NC):
        received(slot_x.at[pl.ds(0, cap * len(near))], tok_rs.at[2 + dc])
        forward([(dy, dc) for dy in near])
        if dc == 0:
            reduce_x(0)
        elif far:
            dispatch(send_c, slot_c, False, direct_order[-2:-1])
    if far:
        received(slot_x.at[pl.ds(0, pair), pl.ds(0, width - share)], far_rs)
        forward([(far, 0), (far, 1)])
    for dy in near:
        reduce_x(dy)

    for copy in loads[5:8]:
        copy.wait()
    all_x = slot_x[...]
    pre = dot_nt(g[...], all_x)
    up = dot_nt(u[...], all_x)
    tang_gate = dot_nt(vg[...], all_x)
    tang_up = dot_nt(vu[...], all_x)
    sig = jax.nn.sigmoid(pre)
    silu = pre * sig
    slope_one = sig * (1.0 + pre * (1.0 - sig))
    slope_two = sig * (1.0 - sig) * (2.0 + pre * (1.0 - 2.0 * sig))
    silu_tang = slope_one * tang_gate
    hidden_tang = (silu_tang * up + silu * tang_up).astype(BF16)

    if far:
        reduce_x(far)
        dispatch(send_c, slot_c, False, direct_order[-1:])

    def piece(xx, zz):
        return mixed.at[:, pl.ds(aligned(xx * (xw // LANES) + zz // NC, LANES), LANES)]

    def gather_z(dz):
        return pltpu.make_async_remote_copy(
            src_ref=piece(x, z), dst_ref=piece(x, z), send_sem=gz_ss,
            recv_sem=gz_rs.at[dz - 1], device_id=device(dz=dz), device_id_type=MESH,
        )

    @pl.when(away == 0)
    def _():
        received(final.at[pl.ds(0, NZ * rows - cap)], fin_rs)
        total = final[pl.ds(0, rows), :].astype(F32)
        for zz in range(1, NZ):
            total = total + final[pl.ds(zz * rows, rows), :].astype(F32)
        returned = total.astype(BF16)
        picked0 = dot_tn(disp[:, :tokens], returned)
        picked1 = dot_tn(disp[:, tokens:], returned)
        piece(x, z)[...] = (prob_t[0] * picked0 + prob_t[1] * picked1).astype(BF16)
        for dz in range(1, NZ):
            gather_z(dz).start()

    def pass_on(number, source=None):
        back = NC * number + (away if source is None else 1 - source)
        zz = (z + NZ - back) % NZ
        part = piece(x, zz)
        if number or not source:
            received(part, gz_rs.at[back - 1])
        for dx in range(1, nx):
            send(part, part, gx_ss, gx_rs, device(dx=dx))

    @pl.when(away == 0)
    def _():
        pass_on(0, True)

    def outer(left, right, target):
        left = left.astype(BF16)
        half = width // 2
        for part in range(2):
            columns = pl.ds(part * half, half)
            target[:, columns] = dot_nn(left, right[:, columns])

    @pl.when(away == 1)
    def _():
        pass_on(0, False)

    for number in (3, 1, 2):
        if number < NZ // NC:
            pass_on(number)

    received(slot_c.at[pl.ds(0, rows - cap)], cot_rs)
    all_c = slot_c[...]
    back_grad = dot_nt(w[...], all_c)
    back_tang = dot_nt(vw[...], all_c)
    outer(hidden_tang, slot_c, hvp_down)
    outer(back_tang * silu + back_grad * silu_tang, slot_x, hvp_up)
    outer(
        (back_tang * up + back_grad * tang_up) * slope_one + back_grad * up * slope_two * tang_gate,
        slot_x, hvp_gate,
    )

    gathered = NZ // NC * (nx - 1) * LANES
    received(mixed.at[:, pl.ds(0, gathered)], gx_rs)

    direct = 1 + NC * len(near)
    sent(slot_x.at[pl.ds(0, direct * cap)], tok_ss)
    sent(slot_c.at[pl.ds(0, rows - cap)], cot_ss)
    if far:
        sent(slot_x.at[pl.ds(0, pair), pl.ds(0, share)], tokf_ss)
        sent(slot_x.at[pl.ds(0, pair), pl.ds(0, width - share)], far_ss)
    sent(xsend, x_ss)
    sent(final.at[pl.ds(0, (ny * NZ - 1) * cap)], fin_ss)
    sent(mixed.at[:, pl.ds(0, gathered)], gx_ss)

    @pl.when(away == 1)
    def _():
        sent(final.at[pl.ds(0, cap)], own_ss)

    @pl.when(away == 0)
    def _():
        sent(mixed.at[:, pl.ds(0, (NZ - 1) * LANES)], gz_ss)


def store_kernel(*refs):
    *arrays, sems = refs
    half = len(arrays) // 2
    copies = [
        pltpu.make_async_copy(arrays[i], arrays[half + i], sems.at[i]) for i in range(half)
    ]
    for copy in copies:
        copy.start()
    for copy in copies:
        copy.wait()


def shards(nx, ny, tokens, cotangent, router_logits, routes, *weights):
    count, width = tokens.shape
    hidden = weights[0].shape[1]
    cap = routes.shape[1] * count * 3 // (2 * ny * NC)
    pair = NC * cap
    rows = ny * pair
    xw = width // nx
    weights = [each.reshape(hidden, width) for each in weights]
    dma = pltpu.SemaphoreType.DMA
    vmem = pltpu.VMEM
    any_spec = pl.BlockSpec(memory_space=pl.ANY)
    hbm_spec = pl.BlockSpec(memory_space=pltpu.HBM)
    vmem_spec = pl.BlockSpec(memory_space=pltpu.VMEM)
    sds = jax.ShapeDtypeStruct
    hvp = sds((hidden, width), F32)
    shapes = (sds((count, width), BF16), hvp, hvp, hvp)
    args = (tokens, cotangent, router_logits.T, routes.T, *weights)
    args = [pltpu.with_memory_space_constraint(each, pltpu.HBM) for each in args]
    results = pl.pallas_call(
        functools.partial(layer_kernel, nx, ny, cap),
        out_shape=tuple(pltpu.VMEM(each.shape, each.dtype) for each in shapes),
        in_specs=[hbm_spec] * 10,
        out_specs=[vmem_spec] * 4,
        scratch_shapes=[vmem(args[2].shape, F32), vmem(args[3].shape, jnp.int32)]
        + [vmem((count, width), BF16)] * 2
        + [vmem((hidden, width), BF16)] * 6
        + [vmem((rows, 2 * count), BF16), vmem((2, count, LANES), F32)]
        + [vmem((rows, width), BF16)] * 4
        + [
            vmem((ny, nx - 1, pair, xw), BF16), vmem((ny, nx - 1, pair, xw), BF16),
            vmem((ny, pair, xw), F32), vmem((ny, pair, xw), BF16),
            vmem((NZ * rows, LANES), BF16),
            dma((10,)), dma((9,)), dma((2 + NC,)), dma((ny,)), dma((4,)), dma((NZ - 1,)),
        ],
        compiler_params=pltpu.CompilerParams(
            collective_id=0, has_side_effects=True, vmem_limit_bytes=36 * 1024 * 1024
        ),
    )(*args)
    mixed, *outs = pl.pallas_call(
        store_kernel,
        out_shape=tuple(pltpu.HBM(each.shape, each.dtype) for each in shapes),
        in_specs=[any_spec] * 4,
        out_specs=[hbm_spec] * 4,
        scratch_shapes=[dma((4,))],
        compiler_params=pltpu.CompilerParams(vmem_limit_bytes=1024 * 1024),
    )(*[pltpu.with_memory_space_constraint(each, pltpu.VMEM) for each in results])
    return (mixed, *(each[None] for each in outs))


def solution(mesh):
    ny = mesh.shape["expert"] // NC
    nx = mesh.shape["dp"] // NZ
    row = P("expert", None)
    mat = P("expert", "dp", None)
    return jax.shard_map(
        functools.partial(shards, nx, ny),
        mesh=mesh,
        in_specs=(row,) * 4 + (mat,) * 6,
        out_specs=(row, mat, mat, mat),
        check_vma=False,
    )
```
